32 devices in a mesh: dom: 16 (over z, y, x), grp: 2 (over core).
Axes of the slice: x: 2, y: 2, z: 4, core: 2. Of those that a mesh axis runs over, the one named last changes fastest.
Arguments:
- tangent_tiles: bfloat16 [4096, 128, 128], P(('grp', 'dom')), parts along dimension 0, may hold values from -0.5 to 0.5
- tile_blocks: int32 [2048, 2], P('dom'), may hold values from 0 to 127, as said below
- block_home: int32 [128], replicated, may hold values from 0 to 127, as said below
- tile_count: int32 [16], P('dom'), may hold values from 48 to 128, as said below
- basis: bfloat16 [16384, 256], P('dom'), may hold values from -0.29882812 to 0.29882812
Outputs:
- reduced: float32 [512, 256], P('grp'), parts along dimension 0
The draws below stay inside these ranges and needn't reach their ends.
There are 2 independent parts, one for each index of `grp`. The reference program is written for one: setup_inputs(seed, part) draws one part's arguments, and reference() takes and returns one part's arrays. A program takes and returns all parts, laid end to end along the dimension named above; an argument that names none is the same for every part. Nothing has to cross between parts.
Inputs may be any that keep to these rules, and one draw needn't show every extreme that they name: `tile_blocks`: every row block named by a device's tile slots has its position held by one of the devices with dom index from that device's index - 4 to its index + 8 // 2 - 1, taken cyclically. Among the row blocks named by one device's 128 slots, at most 2 distinct ones have their position held by any one device; every device reaches 2 for some holder. `block_home`: A permutation of the row blocks. `tile_count`: some device has exactly 128 live slots.
All inputs are finite; a program needn't handle non-finite values.
Results may differ from the reference program's by a relative error of at most 0.0029.
Values may be sent and summed in bfloat16 or wider, within the bound.
A program may use at most 64 MiB of HBM per device.

```python
import jax
import jax.numpy as jnp
from jax import lax

BLOCK = 128
RANK = 256
TILE_DEV = 128
BLK_DEV = 8
CAP = 2
NEAR = 8
NB = 128
TILES = 2048
N_DOM = 16


def layout_tables(key):
    home = jax.random.permutation(jax.random.fold_in(key, 11), NB).astype(jnp.int32)
    at_place = jnp.argsort(home, stable=True).astype(jnp.int32)
    device_ids = jnp.arange(N_DOM, dtype=jnp.int32)[:, None, None]
    steps_away = jax.random.randint(jax.random.fold_in(key, 12), (N_DOM, TILE_DEV, 2), 0, NEAR) - NEAR // 2
    owners = (device_ids + steps_away) % N_DOM
    shifts = jax.random.randint(jax.random.fold_in(key, 13), (N_DOM, N_DOM), 0, BLK_DEV)
    picks = jax.random.randint(jax.random.fold_in(key, 14), (N_DOM, TILE_DEV, 2), 0, CAP)
    owners = owners.at[:, 0, 1].set(owners[:, 0, 0])
    picks = picks.at[:, 0, 0].set(0)
    picks = picks.at[:, 0, 1].set(1)
    offset = shifts[device_ids, owners]
    place = owners * BLK_DEV + (offset + picks) % BLK_DEV
    linked = at_place[place].reshape(TILE_DEV * N_DOM, 2).astype(jnp.int32)
    return (home, linked)


def draw_tile_blocks(key, part):
    return layout_tables(key)[1]


def draw_block_home(key, part):
    return layout_tables(key)[0]


def draw_tile_count(key, part):
    counts = jax.random.randint(jax.random.fold_in(key, 21), (N_DOM,), 3 * TILE_DEV // 8, TILE_DEV + 1)
    busiest = jax.random.randint(jax.random.fold_in(key, 22), (), 0, N_DOM)
    counts = jnp.where(jnp.arange(N_DOM) == busiest, TILE_DEV, counts)
    return counts.astype(jnp.int32)


def levels(stream_key, extent, cuts, least, largest):
    gain, own = 1.0, jax.random.fold_in(stream_key, 6)
    for position, parts in cuts:
        steps = jnp.exp(jax.random.uniform(jax.random.fold_in(own, position), (parts,), jnp.float32, least / len(cuts), largest / len(cuts)))
        gain = gain * jnp.repeat(steps, extent[position] // parts).reshape([-1 if axis == position else 1 for axis in range(len(extent))])
    return gain


def gaussian(own_key, dims, width, limit, shards=(), kind=jnp.bfloat16):
    entries = jax.random.normal(own_key, dims, jnp.float32) * width
    if len(shards) > 0:
        entries = levels(own_key, dims, shards, -0.22, 0.18) * entries
    return jnp.clip(entries, min=-limit, max=limit).astype(kind)


def setup_inputs(seed: int = 0, part: int = 0) -> dict:
    arg_keys = jax.random.split(jax.random.key(seed), 6)
    own_keys = jax.random.split(jax.random.fold_in(arg_keys[5], part), 6)
    tangent_tiles = gaussian(own_keys[0], (TILES, BLOCK, BLOCK), BLOCK ** -0.5, 0.5, ((0, 16),))
    tile_blocks = draw_tile_blocks(jax.random.fold_in(arg_keys[5], 71), part)
    block_home = draw_block_home(jax.random.fold_in(arg_keys[5], 71), part)
    tile_count = draw_tile_count(jax.random.fold_in(arg_keys[5], 71), part)
    basis = gaussian(arg_keys[4], (NB * BLOCK, RANK), 0.05, 0.29882812, ((0, 16),))
    return {"tangent_tiles": tangent_tiles, "tile_blocks": tile_blocks, "block_home": block_home, "tile_count": tile_count, "basis": basis}


def reference(tangent_tiles, tile_blocks, block_home, tile_count, basis):
    stored = basis.reshape(NB, BLOCK, RANK)
    blocks = jnp.take(stored, block_home, axis=0)
    tiles = tangent_tiles.reshape(N_DOM, TILE_DEV, BLOCK, BLOCK)
    links = tile_blocks.reshape(N_DOM, TILE_DEV, 2)
    slots = jnp.arange(TILE_DEV, dtype=jnp.int32)

    def one_device(carry, items):
        tile_set, link_set, count = items
        live = (slots < count).astype(jnp.float32)
        cols = jnp.take(blocks, link_set[:, 1], axis=0).astype(jnp.float32)
        rows = jnp.take(blocks, link_set[:, 0], axis=0)
        right = jnp.einsum("tab,tbr->tar", tile_set.astype(jnp.float32), cols)
        right = (right * live[:, None, None]).astype(jnp.bfloat16)
        part = jnp.dot(rows.reshape(TILE_DEV * BLOCK, RANK).T, right.reshape(TILE_DEV * BLOCK, RANK), preferred_element_type=jnp.float32)
        return carry + part, None

    total, _ = lax.scan(one_device, jnp.zeros((RANK, RANK), jnp.float32), (tiles, links, tile_count))
    return total
```

```python
import functools

import jax
import jax.numpy as jnp
from jax import lax
from jax.experimental import pallas as pl
from jax.experimental.pallas import tpu as pltpu
from jax.sharding import PartitionSpec as P

CAP = 2
NEAR = 8
GROUP = 16
LOADS = 4
MESH = pl.DeviceIdType.MESH


def dot(a, b):
    return jnp.dot(a, b, preferred_element_type=jnp.float32)


def within(index, size):
    return jnp.minimum(jnp.maximum(index, 0), size - 1)


def kernel(ndom, ngrp, tb_ref, home_ref, count_ref, basis_ref, tiles_hbm, out_ref,
           tiles, req_out, req_in, req_s, slot_v, slot_s, served, fetched, turned,
           part, rs_in, ag, acc, tile_sem, req_send, req_recv, table_sem, slot_sem,
           blk_send, blk_recv, fwd_send, fwd_recv, rs_send, rs_recv, ag_send, ag_recv):
    me = lax.axis_index("dom")
    grp = lax.axis_index("grp")
    paired = ngrp == CAP
    ntile = tiles.shape[0]
    nblk = home_ref.shape[1]
    blk_dev = nblk // ndom
    half = NEAR // 2
    here = NEAR // 2

    barrier = pltpu.get_barrier_semaphore()
    for s in range(1, ndom):
        peer = lax.rem(me + s, ndom)
        pl.semaphore_signal(barrier, inc=1, device_id={"dom": peer, "grp": grp}, device_id_type=MESH)
    if paired:
        pl.semaphore_signal(barrier, inc=1, device_id={"dom": me, "grp": 1 - grp}, device_id_type=MESH)

    per = ntile // LOADS
    loads = [
        pltpu.make_async_copy(tiles_hbm.at[pl.ds(i * per, per)], tiles.at[pl.ds(i * per, per)], tile_sem.at[i])
        for i in range(LOADS)
    ]
    for load in loads:
        load.start()

    pos = lax.broadcasted_iota(jnp.int32, (nblk, nblk), 0)
    other = lax.broadcasted_iota(jnp.int32, (nblk, nblk), 1)
    moved = jnp.where(pos == home_ref[...], 1.0, 0.0).astype(jnp.bfloat16)
    ids = lax.broadcasted_iota(jnp.int32, (nblk, ntile), 0)
    at_row = dot(moved, jnp.where(ids == tb_ref[0:1, :], 1.0, 0.0).astype(jnp.bfloat16))
    at_col = dot(moved, jnp.where(ids == tb_ref[1:2, :], 1.0, 0.0).astype(jnp.bfloat16))
    wanted = jnp.max(jnp.maximum(at_row, at_col), axis=1, keepdims=True)
    wanted = jnp.broadcast_to(wanted, (nblk, 128))
    before = jnp.where((pos // blk_dev == other // blk_dev) & (other < pos), 1.0, 0.0).astype(jnp.bfloat16)
    order = dot(before, wanted.astype(jnp.bfloat16))
    lane_pos = lax.broadcasted_iota(jnp.int32, (nblk, 128), 0)
    local = lax.rem(lane_pos, blk_dev).astype(jnp.float32)
    near = lax.broadcasted_iota(jnp.int32, (NEAR, nblk), 0)
    near_pos = lax.broadcasted_iota(jnp.int32, (NEAR, nblk), 1)
    holder = lax.rem(near + (me + ndom - half), ndom)
    group = jnp.where(near_pos // blk_dev == holder, 1.0, 0.0).astype(jnp.bfloat16)
    for level in range(CAP):
        chosen = jnp.where(order == float(level), wanted * local, 0.0)
        table = dot(group, chosen.astype(jnp.bfloat16)).astype(jnp.int32)
        for k in range(NEAR):
            req_out[k, level:level + 1, :] = table[k:k + 1, :]
    window = lax.rem(lane_pos // blk_dev + (2 * ndom + half) - me, ndom)
    window = jnp.minimum(window, NEAR - 1)
    slot_map = (window * CAP).astype(jnp.float32) + order
    slot_map = jnp.broadcast_to(slot_map[:, 0:1], (nblk, ntile))
    slot_v[0:1, :] = jnp.sum(at_row * slot_map, axis=0, keepdims=True).astype(jnp.int32)
    slot_v[1:2, :] = jnp.sum(at_col * slot_map, axis=0, keepdims=True).astype(jnp.int32)

    pl.semaphore_wait(barrier, ndom - 1 + (1 if paired else 0))

    steps = [k for k in range(NEAR) if k != here]
    asks = {}
    for k in steps:
        target = lax.rem(me + (k - half + ndom), ndom)
        asks[k] = pltpu.make_async_remote_copy(
            src_ref=req_out.at[k], dst_ref=req_in.at[k], send_sem=req_send.at[k], recv_sem=req_recv.at[k],
            device_id={"dom": target, "grp": grp}, device_id_type=MESH)
        asks[k].start()
    own = pltpu.make_async_copy(req_out.at[here], req_s.at[here], table_sem.at[here])
    own.start()
    slots = pltpu.make_async_copy(slot_v, slot_s, slot_sem)
    slots.start()
    tables = {}
    for k in steps:
        asks[k].wait_recv()
        tables[k] = pltpu.make_async_copy(req_in.at[k], req_s.at[k], table_sem.at[k])
        tables[k].start()

    sends = {}
    for k in steps:
        tables[k].wait()
        asker = lax.rem(me + (half - k + ndom), ndom)
        if paired:
            served[k, 0] = basis_ref[within(req_s[k, grp, 0], blk_dev)]
            sends[k] = [pltpu.make_async_remote_copy(
                src_ref=served.at[k, 0], dst_ref=fetched.at[k * CAP + grp],
                send_sem=blk_send.at[k, 0], recv_sem=blk_recv.at[k, 0],
                device_id={"dom": asker, "grp": grp}, device_id_type=MESH)]
        else:
            for level in range(CAP):
                served[k, level] = basis_ref[within(req_s[k, level, 0], blk_dev)]
            sends[k] = [pltpu.make_async_remote_copy(
                src_ref=served.at[k, level], dst_ref=fetched.at[k * CAP + level],
                send_sem=blk_send.at[k, level], recv_sem=blk_recv.at[k, level],
                device_id={"dom": asker, "grp": grp}, device_id_type=MESH) for level in range(CAP)]
        for send in sends[k]:
            send.start()
    own.wait()
    for level in range(CAP):
        mine = basis_ref[within(req_s[here, level, 0], blk_dev)]
        fetched[here * CAP + level] = mine
        turned[here * CAP + level] = mine.T

    forwards = {}
    for k in steps:
        for send in sends[k]:
            send.wait_recv()
        if paired:
            forwards[k] = pltpu.make_async_remote_copy(
                src_ref=fetched.at[k * CAP + grp], dst_ref=fetched.at[k * CAP + grp],
                send_sem=fwd_send.at[k], recv_sem=fwd_recv.at[k],
                device_id={"dom": me, "grp": 1 - grp}, device_id_type=MESH)
            forwards[k].start()
            turned[k * CAP + grp] = fetched[k * CAP + grp].T
        else:
            for level in range(CAP):
                turned[k * CAP + level] = fetched[k * CAP + level].T
    if paired:
        for k in steps:
            pltpu.make_async_remote_copy(
                src_ref=fetched.at[k * CAP + 1 - grp], dst_ref=fetched.at[k * CAP + 1 - grp],
                send_sem=fwd_send.at[k], recv_sem=fwd_recv.at[k],
                device_id={"dom": me, "grp": 1 - grp}, device_id_type=MESH).wait_recv()
            turned[k * CAP + 1 - grp] = fetched[k * CAP + 1 - grp].T
    for k in steps:
        asks[k].wait_send()
        for send in sends[k]:
            send.wait_send()
        if paired:
            forwards[k].wait_send()
    slots.wait()
    for load in loads:
        load.wait()

    count = count_ref[0]
    acc[...] = jnp.zeros_like(acc)

    def project(step, carry):
        rights, lefts = [], []
        for i in range(GROUP):
            t = step * GROUP + i
            right = dot(tiles[t], fetched[within(slot_s[1, t], NEAR * CAP)])
            live = jnp.where(t < count, 1.0, 0.0)
            rights.append((right * live).astype(jnp.bfloat16))
            lefts.append(turned[within(slot_s[0, t], NEAR * CAP)])
        acc[...] += dot(jnp.concatenate(lefts, axis=1), jnp.concatenate(rights, axis=0))
        return carry

    lax.fori_loop(0, ntile // GROUP, project, 0)

    rows = part.shape[1]
    for j in range(ndom):
        part[j] = acc[j * rows:(j + 1) * rows, :]

    scatters = []
    for s in range(1, ndom):
        peer = lax.rem(me + s, ndom)
        scatters.append(pltpu.make_async_remote_copy(
            src_ref=part.at[peer], dst_ref=rs_in.at[s], send_sem=rs_send.at[s], recv_sem=rs_recv.at[s],
            device_id={"dom": peer, "grp": grp}, device_id_type=MESH))
        scatters[-1].start()
    total = part[me]
    for s in range(1, ndom):
        scatters[s - 1].wait_recv()
        total = total + rs_in[s]
    ag[me] = total.astype(jnp.bfloat16)

    gathers = []
    for s in range(1, ndom):
        peer = lax.rem(me + s, ndom)
        gathers.append(pltpu.make_async_remote_copy(
            src_ref=ag.at[me], dst_ref=ag.at[me], send_sem=ag_send.at[s], recv_sem=ag_recv.at[s],
            device_id={"dom": peer, "grp": grp}, device_id_type=MESH))
        gathers[-1].start()
    for s in range(1, ndom):
        source = lax.rem(me + (ndom - s), ndom)
        pltpu.make_async_remote_copy(
            src_ref=ag.at[source], dst_ref=ag.at[source], send_sem=ag_send.at[s], recv_sem=ag_recv.at[s],
            device_id={"dom": source, "grp": grp}, device_id_type=MESH).wait_recv()
    for j in range(ndom):
        out_ref[j * rows:(j + 1) * rows, :] = ag[j].astype(jnp.float32)
    for s in range(1, ndom):
        scatters[s - 1].wait_send()
        gathers[s - 1].wait_send()


def on_device(ndom, ngrp, tangent_tiles, tile_blocks, block_home, tile_count, basis):
    ntile, block, _ = tangent_tiles.shape
    rank = basis.shape[1]
    nblk = block_home.shape[0]
    blk_dev = basis.shape[0] // block
    rows = rank // ndom
    vmem = pl.BlockSpec(memory_space=pltpu.VMEM)
    bf16, f32, i32 = jnp.bfloat16, jnp.float32, jnp.int32
    dma = pltpu.SemaphoreType.DMA
    return pl.pallas_call(
        functools.partial(kernel, ndom, ngrp),
        out_shape=jax.ShapeDtypeStruct((rank, rank), f32),
        in_specs=[vmem, vmem, pl.BlockSpec(memory_space=pltpu.SMEM), vmem, pl.BlockSpec(memory_space=pl.ANY)],
        out_specs=vmem,
        scratch_shapes=[
            pltpu.VMEM((ntile, block, block), bf16),
            pltpu.VMEM((NEAR, CAP, 128), i32),
            pltpu.VMEM((NEAR, CAP, 128), i32),
            pltpu.SMEM((NEAR, CAP, 128), i32),
            pltpu.VMEM((2, ntile), i32),
            pltpu.SMEM((2, ntile), i32),
            pltpu.VMEM((NEAR, CAP, block, rank), bf16),
            pltpu.VMEM((NEAR * CAP, block, rank), bf16),
            pltpu.VMEM((NEAR * CAP, rank, block), bf16),
            pltpu.VMEM((ndom, rows, rank), f32),
            pltpu.VMEM((ndom, rows, rank), f32),
            pltpu.VMEM((ndom, rows, rank), bf16),
            pltpu.VMEM((rank, rank), f32),
            dma((LOADS,)),
            dma((NEAR,)), dma((NEAR,)), dma((NEAR,)), dma,
            dma((NEAR, CAP)), dma((NEAR, CAP)), dma((NEAR,)), dma((NEAR,)),
            dma((ndom,)), dma((ndom,)), dma((ndom,)), dma((ndom,)),
        ],
        compiler_params=pltpu.CompilerParams(collective_id=0, has_side_effects=True),
    )(tile_blocks.T, block_home.reshape(1, nblk), tile_count, basis.reshape(blk_dev, block, rank), tangent_tiles)


def solution(mesh):
    return jax.shard_map(
        functools.partial(on_device, mesh.shape["dom"], mesh.shape["grp"]),
        mesh=mesh,
        in_specs=(P(("grp", "dom"), None, None), P("dom", None), P(), P("dom"), P("dom", None)),
        out_specs=P("grp", None),
        check_vma=False,
    )
```

```python
import functools

import jax
import jax.numpy as jnp
from jax import lax
from jax.experimental import pallas as pl
from jax.experimental.pallas import tpu as pltpu
from jax.sharding import PartitionSpec as P

CAP = 2
NEAR = 8
GROUP = 32
LOADS = 4
MESH = pl.DeviceIdType.MESH


def dot(a, b):
    return jnp.dot(a, b, preferred_element_type=jnp.float32)


def within(index, size):
    return jnp.minimum(jnp.maximum(index, 0), size - 1)


def kernel(ndom, ngrp, tb_hbm, home_hbm, count_hbm, basis_hbm, tiles_hbm, out_hbm,
           tb_ref, home_ref, count_ref, basis_ref, in_sem, out_sem, tiles, req_out, req_in, req_s, slot_v, slot_s, served, fetched, turned,
           part, rs_in, ag, acc, tile_sem, req_send, req_recv, table_sem, slot_sem,
           blk_send, blk_recv, fwd_send, fwd_recv, rs_send, rs_recv, ag_send, ag_recv):
    me = lax.axis_index("dom")
    grp = lax.axis_index("grp")
    paired = ngrp == CAP
    ntile = tiles.shape[0]
    nblk = home_ref.shape[1]
    blk_dev = nblk // ndom
    half = NEAR // 2
    here = NEAR // 2

    barrier = pltpu.get_barrier_semaphore()
    for s in range(1, ndom):
        peer = lax.rem(me + s, ndom)
        pl.semaphore_signal(barrier, inc=1, device_id={"dom": peer, "grp": grp}, device_id_type=MESH)
    if paired:
        pl.semaphore_signal(barrier, inc=1, device_id={"dom": me, "grp": 1 - grp}, device_id_type=MESH)

    inputs = [
        pltpu.make_async_copy(tb_hbm, tb_ref, in_sem.at[0]),
        pltpu.make_async_copy(home_hbm, home_ref, in_sem.at[1]),
        pltpu.make_async_copy(count_hbm, count_ref, in_sem.at[2]),
        pltpu.make_async_copy(basis_hbm, basis_ref, in_sem.at[3]),
    ]
    for load in inputs:
        load.start()
    per = ntile // LOADS
    loads = [
        pltpu.make_async_copy(tiles_hbm.at[pl.ds(i * per, per)], tiles.at[pl.ds(i * per, per)], tile_sem.at[i])
        for i in range(LOADS)
    ]
    for load in loads:
        load.start()

    for load in inputs[:3]:
        load.wait()
    pos = lax.broadcasted_iota(jnp.int32, (nblk, nblk), 0)
    other = lax.broadcasted_iota(jnp.int32, (nblk, nblk), 1)
    moved = jnp.where(pos == home_ref[...], 1.0, 0.0).astype(jnp.bfloat16)
    ids = lax.broadcasted_iota(jnp.int32, (nblk, ntile), 0)
    at_row = dot(moved, jnp.where(ids == tb_ref[0:1, :], 1.0, 0.0).astype(jnp.bfloat16))
    at_col = dot(moved, jnp.where(ids == tb_ref[1:2, :], 1.0, 0.0).astype(jnp.bfloat16))
    wanted = jnp.max(jnp.maximum(at_row, at_col), axis=1, keepdims=True)
    wanted = jnp.broadcast_to(wanted, (nblk, 128))
    before = jnp.where((pos // blk_dev == other // blk_dev) & (other < pos), 1.0, 0.0).astype(jnp.bfloat16)
    order = dot(before, wanted.astype(jnp.bfloat16))
    lane_pos = lax.broadcasted_iota(jnp.int32, (nblk, 128), 0)
    local = lax.rem(lane_pos, blk_dev).astype(jnp.float32)
    near = lax.broadcasted_iota(jnp.int32, (NEAR, nblk), 0)
    near_pos = lax.broadcasted_iota(jnp.int32, (NEAR, nblk), 1)
    holder = lax.rem(near + (me + ndom - half), ndom)
    group = jnp.where(near_pos // blk_dev == holder, 1.0, 0.0).astype(jnp.bfloat16)
    for level in range(CAP):
        chosen = jnp.where(order == float(level), wanted * local, 0.0)
        table = dot(group, chosen.astype(jnp.bfloat16)).astype(jnp.int32)
        for k in range(NEAR):
            req_out[k, level:level + 1, :] = table[k:k + 1, :]
    window = lax.rem(lane_pos // blk_dev + (2 * ndom + half) - me, ndom)
    window = jnp.minimum(window, NEAR - 1)
    slot_map = (window * CAP).astype(jnp.float32) + order
    slot_map = jnp.broadcast_to(slot_map[:, 0:1], (nblk, ntile))
    row_slot = jnp.sum(at_row * slot_map, axis=0, keepdims=True).astype(jnp.int32)
    live = lax.broadcasted_iota(jnp.int32, (1, ntile), 1) < count_ref[0]
    slot_v[0:1, :] = jnp.where(live, row_slot, NEAR * CAP)
    turned[NEAR * CAP] = jnp.zeros(turned.shape[1:], turned.dtype)
    slot_v[1:2, :] = jnp.sum(at_col * slot_map, axis=0, keepdims=True).astype(jnp.int32)

    pl.semaphore_wait(barrier, ndom - 1 + (1 if paired else 0))

    steps = sorted((k for k in range(NEAR) if k != here), key=lambda k: -abs(k - here))
    asks = {}
    for k in steps:
        target = lax.rem(me + (k - half + ndom), ndom)
        asks[k] = pltpu.make_async_remote_copy(
            src_ref=req_out.at[k], dst_ref=req_in.at[k], send_sem=req_send.at[k], recv_sem=req_recv.at[k],
            device_id={"dom": target, "grp": grp}, device_id_type=MESH)
        asks[k].start()
    own = pltpu.make_async_copy(req_out.at[here], req_s.at[here], table_sem.at[here])
    own.start()
    slots = pltpu.make_async_copy(slot_v, slot_s, slot_sem)
    slots.start()
    tables = {}
    for k in steps:
        asks[k].wait_recv()
        tables[k] = pltpu.make_async_copy(req_in.at[k], req_s.at[k], table_sem.at[k])
        tables[k].start()

    inputs[3].wait()
    sends = {}
    for k in steps:
        tables[k].wait()
        asker = lax.rem(me + (half - k + ndom), ndom)
        if paired:
            served[k, 0] = basis_ref[within(req_s[k, grp, 0], blk_dev)]
            sends[k] = [pltpu.make_async_remote_copy(
                src_ref=served.at[k, 0], dst_ref=fetched.at[k * CAP + grp],
                send_sem=blk_send.at[k, 0], recv_sem=blk_recv.at[k, 0],
                device_id={"dom": asker, "grp": grp}, device_id_type=MESH)]
        else:
            for level in range(CAP):
                served[k, level] = basis_ref[within(req_s[k, level, 0], blk_dev)]
            sends[k] = [pltpu.make_async_remote_copy(
                src_ref=served.at[k, level], dst_ref=fetched.at[k * CAP + level],
                send_sem=blk_send.at[k, level], recv_sem=blk_recv.at[k, level],
                device_id={"dom": asker, "grp": grp}, device_id_type=MESH) for level in range(CAP)]
        for send in sends[k]:
            send.start()
    own.wait()
    for level in range(CAP):
        mine = basis_ref[within(req_s[here, level, 0], blk_dev)]
        fetched[here * CAP + level] = mine
        turned[here * CAP + level] = mine.T

    forwards = {}
    for k in steps:
        for send in sends[k]:
            send.wait_recv()
        if paired:
            forwards[k] = pltpu.make_async_remote_copy(
                src_ref=fetched.at[k * CAP + grp], dst_ref=fetched.at[k * CAP + grp],
                send_sem=fwd_send.at[k], recv_sem=fwd_recv.at[k],
                device_id={"dom": me, "grp": 1 - grp}, device_id_type=MESH)
            forwards[k].start()
            turned[k * CAP + grp] = fetched[k * CAP + grp].T
        else:
            for level in range(CAP):
                turned[k * CAP + level] = fetched[k * CAP + level].T
    if paired:
        for k in steps:
            pltpu.make_async_remote_copy(
                src_ref=fetched.at[k * CAP + 1 - grp], dst_ref=fetched.at[k * CAP + 1 - grp],
                send_sem=fwd_send.at[k], recv_sem=fwd_recv.at[k],
                device_id={"dom": me, "grp": 1 - grp}, device_id_type=MESH).wait_recv()
            turned[k * CAP + 1 - grp] = fetched[k * CAP + 1 - grp].T
    for k in steps:
        asks[k].wait_send()
        for send in sends[k]:
            send.wait_send()
        if paired:
            forwards[k].wait_send()
    slots.wait()
    for load in loads:
        load.wait()

    acc[...] = jnp.zeros_like(acc)

    def project(step, carry):
        rights, lefts = [], []
        for i in range(GROUP):
            t = step * GROUP + i
            right = dot(tiles[t], fetched[within(slot_s[1, t], NEAR * CAP)])
            rights.append(right.astype(jnp.bfloat16))
            lefts.append(turned[within(slot_s[0, t], NEAR * CAP + 1)])
        acc[...] += dot(jnp.concatenate(lefts, axis=1), jnp.concatenate(rights, axis=0))
        return carry

    lax.fori_loop(0, ntile // GROUP, project, 0)

    rows = part.shape[1]
    for j in range(ndom):
        part[j] = acc[j * rows:(j + 1) * rows, :]

    scatters = []
    for s in range(1, ndom):
        peer = lax.rem(me + s, ndom)
        scatters.append(pltpu.make_async_remote_copy(
            src_ref=part.at[peer], dst_ref=rs_in.at[s], send_sem=rs_send.at[s], recv_sem=rs_recv.at[s],
            device_id={"dom": peer, "grp": grp}, device_id_type=MESH))
        scatters[-1].start()
    total = part[me]
    for s in range(1, ndom):
        scatters[s - 1].wait_recv()
        total = total + rs_in[s]
    ag[me] = total.astype(jnp.bfloat16)

    gathers = []
    for s in range(1, ndom):
        peer = lax.rem(me + s, ndom)
        gathers.append(pltpu.make_async_remote_copy(
            src_ref=ag.at[me], dst_ref=ag.at[me], send_sem=ag_send.at[s], recv_sem=ag_recv.at[s],
            device_id={"dom": peer, "grp": grp}, device_id_type=MESH))
        gathers[-1].start()
    for s in range(1, ndom):
        source = lax.rem(me + (ndom - s), ndom)
        pltpu.make_async_remote_copy(
            src_ref=ag.at[source], dst_ref=ag.at[source], send_sem=ag_send.at[s], recv_sem=ag_recv.at[s],
            device_id={"dom": source, "grp": grp}, device_id_type=MESH).wait_recv()
    result = pltpu.make_async_copy(ag, out_hbm, out_sem)
    result.start()
    for s in range(1, ndom):
        scatters[s - 1].wait_send()
        gathers[s - 1].wait_send()
    result.wait()


def on_device(ndom, ngrp, tangent_tiles, tile_blocks, block_home, tile_count, basis):
    ntile, block, _ = tangent_tiles.shape
    rank = basis.shape[1]
    nblk = block_home.shape[0]
    blk_dev = basis.shape[0] // block
    rows = rank // ndom
    whole = pl.BlockSpec(memory_space=pl.ANY)
    bf16, f32, i32 = jnp.bfloat16, jnp.float32, jnp.int32
    dma = pltpu.SemaphoreType.DMA
    reduced = pl.pallas_call(
        functools.partial(kernel, ndom, ngrp),
        out_shape=jax.ShapeDtypeStruct((ndom, rows, rank), bf16),
        in_specs=[whole] * 5,
        out_specs=whole,
        scratch_shapes=[
            pltpu.VMEM((2, ntile), i32),
            pltpu.VMEM((1, nblk), i32),
            pltpu.SMEM((1,), i32),
            pltpu.VMEM((blk_dev, block, rank), bf16),
            dma((4,)), dma,
            pltpu.VMEM((ntile, block, block), bf16),
            pltpu.VMEM((NEAR, CAP, 128), i32),
            pltpu.VMEM((NEAR, CAP, 128), i32),
            pltpu.SMEM((NEAR, CAP, 128), i32),
            pltpu.VMEM((2, ntile), i32),
            pltpu.SMEM((2, ntile), i32),
            pltpu.VMEM((NEAR, CAP, block, rank), bf16),
            pltpu.VMEM((NEAR * CAP, block, rank), bf16),
            pltpu.VMEM((NEAR * CAP + 1, rank, block), bf16),
            pltpu.VMEM((ndom, rows, rank), f32),
            pltpu.VMEM((ndom, rows, rank), f32),
            pltpu.VMEM((ndom, rows, rank), bf16),
            pltpu.VMEM((rank, rank), f32),
            dma((LOADS,)),
            dma((NEAR,)), dma((NEAR,)), dma((NEAR,)), dma,
            dma((NEAR, CAP)), dma((NEAR, CAP)), dma((NEAR,)), dma((NEAR,)),
            dma((ndom,)), dma((ndom,)), dma((ndom,)), dma((ndom,)),
        ],
        compiler_params=pltpu.CompilerParams(collective_id=0, has_side_effects=True),
    )(tile_blocks.T, block_home.reshape(1, nblk), tile_count,
      basis.reshape(blk_dev, block, rank), tangent_tiles)
    return reduced.reshape(rank, rank).astype(f32)


def solution(mesh):
    return jax.shard_map(
        functools.partial(on_device, mesh.shape["dom"], mesh.shape["grp"]),
        mesh=mesh,
        in_specs=(P(("grp", "dom"), None, None), P("dom", None), P(), P("dom"), P("dom", None)),
        out_specs=P("grp", None),
        check_vma=False,
    )
```
